32 devices in a mesh: rep: 8 (over y, x, core), fsdp: 4 (over z).
Axes of the slice: x: 2, y: 2, z: 4, core: 2. Of those that a mesh axis runs over, the one named last changes fastest.
Arguments:
- queries: bfloat16 [4096, 4096], P(('rep', 'fsdp')), may hold values from -18 to 18
- resp_keys: bfloat16 [4096, 512], P(('rep', 'fsdp')), may hold values from -6 to 6
- resp_values: bfloat16 [4096, 512], P(('rep', 'fsdp')), may hold values from -6 to 6
- attn_out: bfloat16 [4096, 4096], P(('rep', 'fsdp')), may hold values from -1.796875 to 1.796875
- out_grad: bfloat16 [4096, 4096], P(('rep', 'fsdp')), may hold values from -24 to 24
- lengths: int32 [32], P(('rep', 'fsdp')), may hold values from 1 to 128, 2560 in all
- prefix_keys: bfloat16 [64, 512], P('fsdp'), may hold values from -18 to 18
- prefix_values: bfloat16 [64, 512], P('fsdp'), may hold values from -6 to 6
Outputs:
- query_grad: bfloat16 [4096, 4096], P(('rep', 'fsdp'))
- key_grad: bfloat16 [4096, 512], P(('rep', 'fsdp'))
- value_grad: bfloat16 [4096, 512], P(('rep', 'fsdp'))
- prefix_key_grad: float32 [64, 512], P('fsdp')
- prefix_value_grad: float32 [64, 512], P('fsdp')
The draws below stay inside these ranges and needn't reach their ends.
Inputs may be any that keep to these rules, and one draw needn't show every extreme that they name: The largest of lengths is exactly 128.
All inputs are finite; a program needn't handle non-finite values. No bound on the sum of `lengths` on one device may be relied on, other than what follows from the above.
Results may differ from the reference program's by a relative error of at most 0.0078.
Values may be sent and summed in bfloat16 or wider, within the bound.
A program may use at most 64 MiB of HBM per device.

```python
import math
import jax
import jax.numpy as jnp
import numpy as np
from jax import lax

HEAD_DIM = 128
Q_HEADS = 32
KV_HEADS = 4
RESP_DEV = 128
TOKENS = 4096
PREFIX = 64
N_REP = 8
N_FSDP = 4


def draw_queries(key, part):
    drawn = jnp.clip(jax.random.normal(jax.random.fold_in(key, 11), (TOKENS, Q_HEADS * HEAD_DIM), jnp.float32), -6.0, 6.0)
    return drawn.astype(jnp.bfloat16)


def draw_prefix_keys(key, part):
    drawn = jnp.clip(jax.random.normal(jax.random.fold_in(key, 13), (PREFIX, KV_HEADS * HEAD_DIM), jnp.float32), -6.0, 6.0)
    return drawn.astype(jnp.bfloat16)


def block_levels(rng, dims, cuts, smallest, top_value):
    level = 1.0
    for position, parts in cuts:
        draws = jax.random.uniform(jax.random.fold_in(jax.random.fold_in(rng, 6), position), (parts,), jnp.float32, smallest / len(cuts), top_value / len(cuts))
        level = level * jnp.repeat(jnp.exp(draws), dims[position] // parts).reshape((-1,) + (1,) * (len(dims) - 1 - position))
    return level


def profile(count, total, limit, skew):
    loads = [(1 << 20) // math.isqrt(grade ** skew) + 1 for grade in range(2, count + 1)]
    spare, holding = total - limit - (count - 1), [1] * (count - 1)
    while spare > 0:
        candidates = [i for i in range(count - 1) if holding[i] < limit]
        mass, budget = sum([loads[i] for i in candidates]), spare
        for i in candidates:
            more = min(limit - holding[i], max(1, budget * loads[i] // mass), spare)
            holding[i] = holding[i] + more
            spare = spare - more
    return np.array([limit] + holding)


def ragged(stream_key, number_of, total, limit, slope):
    if number_of == 2:
        one = jax.random.randint(stream_key, (), max(1, total - limit), min(limit, total - 1) + 1)
        return jnp.stack([one, total - one])
    sizes = jnp.asarray(profile(number_of, total, limit, slope), jnp.int32)
    twos = (number_of - 1) // 2
    donor, taker = sizes[1:1 + 2 * twos:2], sizes[2:2 + 2 * twos:2]
    margin = jnp.minimum(donor - 1, limit - taker)
    passed = jax.random.randint(jax.random.fold_in(stream_key, 1), (twos,), 0, 1 << 20) % (margin + 1)
    sizes = sizes.at[1:1 + 2 * twos:2].set(donor - passed).at[2:2 + 2 * twos:2].set(taker + passed)
    return sizes[jax.random.permutation(jax.random.fold_in(stream_key, 2), number_of)]


def normal_values(key, extent, scale, reach, cuts=(), held_as=jnp.bfloat16):
    gain = block_levels(key, extent, cuts, -0.22, 0.18) if cuts else 1.0
    result = jax.random.normal(key, extent, jnp.float32) * scale * gain
    return jnp.minimum(jnp.maximum(result, -reach), reach).astype(held_as)


def setup_inputs(seed: int = 0) -> dict:
    splits = jax.random.split(jax.random.key(seed), 9)
    return {
        "queries": draw_queries(jax.random.fold_in(splits[8], 71), 0),
        "resp_keys": normal_values(splits[1], (TOKENS, KV_HEADS * HEAD_DIM), 1.0, 6.0, ((0, 32),)),
        "resp_values": normal_values(splits[2], (TOKENS, KV_HEADS * HEAD_DIM), 1.0, 6.0, ((0, 32),)),
        "attn_out": normal_values(splits[3], (TOKENS, Q_HEADS * HEAD_DIM), 0.3, 1.796875, ((0, 32),)),
        "out_grad": normal_values(splits[4], (TOKENS, Q_HEADS * HEAD_DIM), 4.0, 24.0, ((0, 32),)),
        "lengths": ragged(splits[5], N_REP * N_FSDP, N_REP * N_FSDP * RESP_DEV * 5 // 8, RESP_DEV, 1).astype(jnp.int32),
        "prefix_keys": draw_prefix_keys(jax.random.fold_in(splits[8], 71), 0),
        "prefix_values": normal_values(splits[7], (PREFIX, KV_HEADS * HEAD_DIM), 1.0, 6.0, ((0, 4),)),
    }


masked_fill = -1e30


def rounded(values):
    return lax.optimization_barrier(values.astype(jnp.bfloat16)).astype(jnp.float32)


def device_grads(queries, resp_keys, resp_values, attn_out, out_grad, length, prefix_keys, prefix_values):
    resp_rows = queries.shape[0]
    prefix_rows = prefix_keys.shape[0]
    key_count = prefix_rows + resp_rows
    all_keys = jnp.concatenate([prefix_keys, resp_keys], axis=0)
    all_values = jnp.concatenate([prefix_values, resp_values], axis=0)
    row_index = jnp.arange(resp_rows, dtype=jnp.int32)[:, None]
    col_index = jnp.arange(key_count, dtype=jnp.int32)[None, :]
    live_rows = row_index < length
    visible = live_rows & ((col_index < prefix_rows) | (col_index - prefix_rows <= row_index))
    dead_rows = 1.0 - live_rows.astype(jnp.float32)
    group_size = Q_HEADS // KV_HEADS
    score_scale = HEAD_DIM ** -0.5
    block_width = group_size * HEAD_DIM
    query_parts = []
    key_parts = []
    value_parts = []
    for group_index in range(KV_HEADS):
        lower = group_index * block_width
        q_block = queries[:, lower:lower + block_width].reshape(resp_rows, group_size, HEAD_DIM).astype(jnp.float32)
        out_block = attn_out[:, lower:lower + block_width].reshape(resp_rows, group_size, HEAD_DIM).astype(jnp.float32)
        grad_block = out_grad[:, lower:lower + block_width].reshape(resp_rows, group_size, HEAD_DIM).astype(jnp.float32)
        key_block = all_keys[:, group_index * HEAD_DIM:(group_index + 1) * HEAD_DIM].astype(jnp.float32)
        value_block = all_values[:, group_index * HEAD_DIM:(group_index + 1) * HEAD_DIM].astype(jnp.float32)
        scores = jnp.einsum("rhd,kd->hrk", q_block, key_block) * score_scale
        scores = jnp.where(visible[None], scores, masked_fill)
        row_max = jnp.max(scores, axis=2, keepdims=True)
        shifted = jnp.where(visible[None], jnp.exp(scores - row_max), 0.0)
        denominator = jnp.sum(shifted, axis=2, keepdims=True) + dead_rows[None]
        log_total = row_max + jnp.log(denominator)
        attn_prob = jnp.where(visible[None], jnp.exp(scores - log_total), 0.0)
        value_part = jnp.einsum("hrk,rhd->kd", rounded(attn_prob), grad_block)
        prob_grad = jnp.einsum("rhd,kd->hrk", grad_block, value_block)
        row_delta = jnp.einsum("rhd,rhd->hr", grad_block, out_block)
        score_half = rounded(attn_prob * (prob_grad - row_delta[:, :, None]))
        query_part = jnp.einsum("hrk,kd->rhd", score_half, key_block) * score_scale
        key_part = jnp.einsum("hrk,rhd->kd", score_half, q_block) * score_scale
        query_parts.append(query_part.reshape(resp_rows, block_width))
        key_parts.append(key_part)
        value_parts.append(value_part)
    query_grad = jnp.concatenate(query_parts, axis=1).astype(jnp.bfloat16)
    key_whole = jnp.concatenate(key_parts, axis=1)
    value_whole = jnp.concatenate(value_parts, axis=1)
    return (query_grad, key_whole[prefix_rows:].astype(jnp.bfloat16), value_whole[prefix_rows:].astype(jnp.bfloat16),
            key_whole[:prefix_rows], value_whole[:prefix_rows])


def reference(queries, resp_keys, resp_values, attn_out, out_grad, lengths, prefix_keys, prefix_values):
    device_count = N_REP * N_FSDP

    def split_rows(array):
        return array.reshape(device_count, RESP_DEV, array.shape[1])

    def device_step(carried, pieces):
        query_dev, key_dev, value_dev, out_dev, grad_dev, length = pieces
        results = device_grads(query_dev, key_dev, value_dev, out_dev, grad_dev, length, prefix_keys, prefix_values)
        return (carried[0] + results[3], carried[1] + results[4]), (results[0], results[1], results[2])

    zero_sums = jnp.zeros((PREFIX, KV_HEADS * HEAD_DIM), jnp.float32)
    sums, grads = lax.scan(device_step, (zero_sums, zero_sums),
                           (split_rows(queries), split_rows(resp_keys), split_rows(resp_values),
                            split_rows(attn_out), split_rows(out_grad), lengths))
    return (grads[0].reshape(TOKENS, Q_HEADS * HEAD_DIM), grads[1].reshape(TOKENS, KV_HEADS * HEAD_DIM),
            grads[2].reshape(TOKENS, KV_HEADS * HEAD_DIM), sums[0], sums[1])
```

```python
import functools

import jax
import jax.numpy as jnp
from jax import lax
from jax.experimental import pallas as pl
from jax.experimental.pallas import tpu as pltpu
from jax.sharding import PartitionSpec as P

HEAD_DIM = 128
Q_HEADS = 32
KV_HEADS = 4
GROUP = Q_HEADS // KV_HEADS
WIDTH = GROUP * HEAD_DIM
SCALE = HEAD_DIM ** (-0.5)
MASKED = -1e30
LAG = 2
PAIR = 2

MESH = pl.DeviceIdType.MESH
F32 = jnp.float32
BF16 = jnp.bfloat16


def dot(a, b, contract):
    return lax.dot_general(a, b, (contract, ((), ())), preferred_element_type=F32)


def kernel(
    n_rep, n_fsdp,
    q_hbm, k_hbm, v_hbm, o_hbm, do_hbm, len_ref, pk_hbm, pv_hbm,
    qg_out, kg_out, vg_out, pk_out, pv_out,
    qb, ob, db, kb, vb, kvp, prob, score, zsend, zrecv, rbuf,
    in_sem, pre_sem, ag_send, ag_recv, z_ssem, z_rsem, r_ssem, r_rsem,
):
    rep, fs = lax.axis_index("rep"), lax.axis_index("fsdp")
    rows = qb.shape[1]
    pre_rows = kvp.shape[3]
    prefix = n_fsdp * pre_rows

    def rep_at(d):
        return lax.rem(rep + d, n_rep)

    def fs_at(d):
        return lax.rem(fs + d, n_fsdp)

    for i, src in enumerate((pk_hbm, pv_hbm)):
        for g in range(KV_HEADS):
            pltpu.make_async_copy(
                src.at[:, pl.ds(g * HEAD_DIM, HEAD_DIM)], kvp.at[fs, g, i], pre_sem.at[i, g]
            ).start()
    barrier = pltpu.get_barrier_semaphore()
    for d in range(1, n_fsdp):
        pl.semaphore_signal(barrier, inc=1, device_id=(rep, fs_at(d)), device_id_type=MESH)
    for d in range(1, n_rep):
        pl.semaphore_signal(barrier, inc=1, device_id=(rep_at(d), fs), device_id_type=MESH)
    loads = ((q_hbm, qb, WIDTH), (do_hbm, db, WIDTH), (o_hbm, ob, WIDTH),
             (k_hbm, kb, HEAD_DIM), (v_hbm, vb, HEAD_DIM))
    for g in range(KV_HEADS):
        for i, (src, dst, width) in enumerate(loads):
            pltpu.make_async_copy(
                src.at[:, pl.ds(g * width, width)], dst.at[g], in_sem.at[g, i]
            ).start()
    for i in range(2):
        for g in range(KV_HEADS):
            pltpu.make_async_copy(kvp.at[fs, g, i], kvp.at[fs, g, i], pre_sem.at[i, g]).wait()
    pl.semaphore_wait(barrier, n_fsdp + n_rep - 2)

    def gather(d):
        return pltpu.make_async_remote_copy(
            src_ref=kvp.at[fs], dst_ref=kvp.at[fs], send_sem=ag_send.at[d - 1],
            recv_sem=ag_recv.at[d - 1], device_id=(rep, fs_at(d)), device_id_type=MESH)

    def scatter(g, d):
        return pltpu.make_async_remote_copy(
            src_ref=zsend.at[g, fs_at(d)], dst_ref=zrecv.at[g, fs], send_sem=z_ssem.at[g, d - 1],
            recv_sem=z_rsem.at[g, d - 1], device_id=(rep, fs_at(d)), device_id_type=MESH)

    def spread(g, d):
        return pltpu.make_async_remote_copy(
            src_ref=rbuf.at[g, rep], dst_ref=rbuf.at[g, rep], send_sem=r_ssem.at[g, d - 1],
            recv_sem=r_rsem.at[g, d - 1], device_id=(rep_at(d), fs), device_id_type=MESH)

    for d in range(1, n_fsdp):
        gather(d).start()

    length = len_ref[0]
    lanes = PAIR * HEAD_DIM if rows == HEAD_DIM else PAIR * rows
    lane = lax.broadcasted_iota(jnp.int32, (rows, lanes), 1)
    pos = lax.rem(lane, rows)
    causal = lax.broadcasted_iota(jnp.int32, (rows, lanes), 0) <= pos
    live = lax.rem(lax.broadcasted_iota(jnp.int32, (1, lanes), 1), rows) < length
    low_half = lax.broadcasted_iota(jnp.int32, (lanes, HEAD_DIM), 1) < HEAD_DIM // 2
    minus = jnp.full((prefix + rows, HEAD_DIM), -1.0, BF16)

    for d in range(1, n_fsdp):
        own = kvp.at[fs_at(n_fsdp - d)]
        pltpu.make_async_copy(own, own, ag_recv.at[d - 1]).wait()

    def reduce_rows(g):
        for d in range(1, n_fsdp):
            slot = zrecv.at[g, fs_at(n_fsdp - d)]
            pltpu.make_async_copy(slot, slot, z_rsem.at[g, d - 1]).wait()
        zrecv[g, fs] = zsend[g, fs]
        total = zrecv[g, 0]
        for i in range(1, n_fsdp):
            total = total + zrecv[g, i]
        rbuf[g, rep] = total
        for d in range(1, n_rep):
            spread(g, d).start()

    def group(g, carry):
        for i, (_, dst, _) in enumerate(loads):
            pltpu.make_async_copy(dst.at[g], dst.at[g], in_sem.at[g, i]).wait()
        keys = jnp.concatenate([kvp[:, g, 0].reshape(prefix, HEAD_DIM), kb[g]], axis=0)
        values = jnp.concatenate([kvp[:, g, 1].reshape(prefix, HEAD_DIM), vb[g]], axis=0)
        values_ext = jnp.concatenate([values, minus], axis=1)

        def heads(ref, first, count):
            return jnp.concatenate(
                [ref[g, :, h * HEAD_DIM:(h + 1) * HEAD_DIM] for h in range(first, first + count)],
                axis=0)

        for c in range(GROUP // PAIR):
            q = heads(qb, c * PAIR, PAIR)
            do = heads(db, c * PAIR, PAIR)
            o = heads(ob, c * PAIR, PAIR)
            prod = do.astype(F32) * o.astype(F32)
            both = prod + pltpu.roll(prod, HEAD_DIM // 2, 1)
            rest = both - both.astype(BF16).astype(F32)
            delta = jnp.where(low_half, both, rest).astype(BF16)
            s = dot(keys, q, ((1,), (1,)))
            dp = dot(values_ext, jnp.concatenate([do, delta], axis=1), ((1,), (1,)))
            s = jnp.concatenate(
                [s[:prefix], jnp.where(causal, s[prefix:], MASKED)], axis=0)
            top = jnp.max(s, axis=0, keepdims=True)
            e = jnp.exp((s - top) * SCALE)
            inv = jnp.where(live, 1.0 / jnp.sum(e, axis=0, keepdims=True), 0.0)
            p = e * inv
            prob[:, c * lanes:(c + 1) * lanes] = p.astype(BF16)
            ds = (p * dp).astype(BF16)
            score[:, c * lanes:(c + 1) * lanes] = ds
            dq = (dot(ds, keys, ((0,), (0,))) * SCALE).astype(BF16)
            for j in range(PAIR):
                at = pl.multiple_of(g * WIDTH + (c * PAIR + j) * HEAD_DIM, HEAD_DIM)
                qg_out[:, pl.ds(at, HEAD_DIM)] = dq[j * rows:(j + 1) * rows]
        dv = dot(prob[...], heads(db, 0, GROUP), ((1,), (0,)))
        dk = dot(score[...], heads(qb, 0, GROUP), ((1,), (0,))) * SCALE
        zsend[g, :, 0] = dk[:prefix].reshape(n_fsdp, pre_rows, HEAD_DIM)
        zsend[g, :, 1] = dv[:prefix].reshape(n_fsdp, pre_rows, HEAD_DIM)
        for d in range(1, n_fsdp):
            scatter(g, d).start()
        at = pl.multiple_of(g * HEAD_DIM, HEAD_DIM)
        kg_out[:, pl.ds(at, HEAD_DIM)] = dk[prefix:].astype(BF16)
        vg_out[:, pl.ds(at, HEAD_DIM)] = dv[prefix:].astype(BF16)

        @pl.when(g >= LAG)
        def _():
            reduce_rows(g - LAG)

        return carry

    lax.fori_loop(0, KV_HEADS, group, 0)
    for g in range(KV_HEADS - LAG, KV_HEADS):
        reduce_rows(g)
    for g in range(KV_HEADS):
        for d in range(1, n_rep):
            slot = rbuf.at[g, rep_at(n_rep - d)]
            pltpu.make_async_copy(slot, slot, r_rsem.at[g, d - 1]).wait()
        total = rbuf[g, 0]
        for i in range(1, n_rep):
            total = total + rbuf[g, i]
        pk_out[:, g * HEAD_DIM:(g + 1) * HEAD_DIM] = total[0]
        pv_out[:, g * HEAD_DIM:(g + 1) * HEAD_DIM] = total[1]
    for d in range(1, n_fsdp):
        gather(d).wait_send()
    for g in range(KV_HEADS):
        for d in range(1, n_fsdp):
            scatter(g, d).wait_send()
        for d in range(1, n_rep):
            spread(g, d).wait_send()


def on_device(n_rep, n_fsdp, q, k, v, o, do, lengths, pk, pv):
    rows = q.shape[0]
    pre_rows = pk.shape[0]
    keys = n_fsdp * pre_rows + rows
    any_ = pl.BlockSpec(memory_space=pl.ANY)
    vmem = pl.BlockSpec(memory_space=pltpu.VMEM)
    dma = pltpu.SemaphoreType.DMA
    piece = (2, pre_rows, HEAD_DIM)
    return pl.pallas_call(
        functools.partial(kernel, n_rep, n_fsdp),
        out_shape=(
            jax.ShapeDtypeStruct(q.shape, BF16),
            jax.ShapeDtypeStruct(k.shape, BF16),
            jax.ShapeDtypeStruct(v.shape, BF16),
            jax.ShapeDtypeStruct(pk.shape, F32),
            jax.ShapeDtypeStruct(pv.shape, F32),
        ),
        in_specs=[any_] * 5 + [pl.BlockSpec(memory_space=pltpu.SMEM)] + [any_] * 2,
        out_specs=(vmem,) * 5,
        scratch_shapes=[
            pltpu.VMEM((KV_HEADS, rows, WIDTH), BF16),
            pltpu.VMEM((KV_HEADS, rows, WIDTH), BF16),
            pltpu.VMEM((KV_HEADS, rows, WIDTH), BF16),
            pltpu.VMEM((KV_HEADS, rows, HEAD_DIM), BF16),
            pltpu.VMEM((KV_HEADS, rows, HEAD_DIM), BF16),
            pltpu.VMEM((n_fsdp, KV_HEADS) + piece, BF16),
            pltpu.VMEM((keys, GROUP * rows), BF16),
            pltpu.VMEM((keys, GROUP * rows), BF16),
            pltpu.VMEM((KV_HEADS, n_fsdp) + piece, F32),
            pltpu.VMEM((KV_HEADS, n_fsdp) + piece, F32),
            pltpu.VMEM((KV_HEADS, n_rep) + piece, F32),
            dma((KV_HEADS, 5)),
            dma((2, KV_HEADS)),
            dma((n_fsdp - 1,)),
            dma((n_fsdp - 1,)),
            dma((KV_HEADS, n_fsdp - 1)),
            dma((KV_HEADS, n_fsdp - 1)),
            dma((KV_HEADS, n_rep - 1)),
            dma((KV_HEADS, n_rep - 1)),
        ],
        compiler_params=pltpu.CompilerParams(collective_id=0, has_side_effects=True),
    )(q, k, v, o, do, lengths, pk, pv)


def solution(mesh):
    wide = P(("rep", "fsdp"), None)
    return jax.shard_map(
        functools.partial(on_device, mesh.shape["rep"], mesh.shape["fsdp"]),
        mesh=mesh,
        in_specs=(wide,) * 5 + (P(("rep", "fsdp")), P("fsdp", None), P("fsdp", None)),
        out_specs=(wide,) * 3 + (P("fsdp", None), P("fsdp", None)),
        check_vma=False,
    )
```

```python
import functools

import jax
import jax.numpy as jnp
from jax import lax
from jax.experimental import pallas as pl
from jax.experimental.pallas import tpu as pltpu
from jax.sharding import PartitionSpec as P

HEAD_DIM = 128
Q_HEADS = 32
KV_HEADS = 4
GROUP = Q_HEADS // KV_HEADS
WIDTH = GROUP * HEAD_DIM
SCALE = HEAD_DIM ** (-0.5)
MASKED = -1e30
LAG = 2
PAIR = 2

MESH = pl.DeviceIdType.MESH
F32 = jnp.float32
BF16 = jnp.bfloat16


def dot(a, b, contract):
    return lax.dot_general(a, b, (contract, ((), ())), preferred_element_type=F32)


def kernel(
    n_rep, n_fsdp,
    q_hbm, k_hbm, v_hbm, o_hbm, do_hbm, len_ref, pk_hbm, pv_hbm,
    qg_out, kg_out, vg_out, pk_out, pv_out,
    qb, ob, db, kb, vb, kvp, prob, score, zsend, zrecv, rbuf,
    in_sem, pre_sem, ag_send, ag_recv, z_ssem, z_rsem, r_ssem, r_rsem,
):
    rep, fs = lax.axis_index("rep"), lax.axis_index("fsdp")
    rows = qb.shape[1]
    pre_rows = kvp.shape[3]
    prefix = n_fsdp * pre_rows

    def rep_at(d):
        return lax.rem(rep + d, n_rep)

    def fs_at(d):
        return lax.rem(fs + d, n_fsdp)

    for i, src in enumerate((pk_hbm, pv_hbm)):
        for g in range(KV_HEADS):
            pltpu.make_async_copy(
                src.at[:, pl.ds(g * HEAD_DIM, HEAD_DIM)], kvp.at[fs, g, i], pre_sem.at[i, g]
            ).start()
    barrier = pltpu.get_barrier_semaphore()
    for d in range(1, n_fsdp):
        pl.semaphore_signal(barrier, inc=1, device_id=(rep, fs_at(d)), device_id_type=MESH)
    for d in range(1, n_rep):
        pl.semaphore_signal(barrier, inc=1, device_id=(rep_at(d), fs), device_id_type=MESH)
    loads = ((q_hbm, qb, WIDTH), (do_hbm, db, WIDTH), (o_hbm, ob, WIDTH),
             (k_hbm, kb, HEAD_DIM), (v_hbm, vb, HEAD_DIM))
    for g in range(KV_HEADS):
        for i, (src, dst, width) in enumerate(loads):
            pltpu.make_async_copy(
                src.at[:, pl.ds(g * width, width)], dst.at[g], in_sem.at[g, i]
            ).start()
    for i in range(2):
        for g in range(KV_HEADS):
            pltpu.make_async_copy(kvp.at[fs, g, i], kvp.at[fs, g, i], pre_sem.at[i, g]).wait()
    pl.semaphore_wait(barrier, n_fsdp + n_rep - 2)

    def gather(d):
        return pltpu.make_async_remote_copy(
            src_ref=kvp.at[fs], dst_ref=kvp.at[fs], send_sem=ag_send.at[d - 1],
            recv_sem=ag_recv.at[d - 1], device_id=(rep, fs_at(d)), device_id_type=MESH)

    def scatter(g, d):
        return pltpu.make_async_remote_copy(
            src_ref=zsend.at[g, fs_at(d)], dst_ref=zrecv.at[g, fs], send_sem=z_ssem.at[g, d - 1],
            recv_sem=z_rsem.at[g, d - 1], device_id=(rep, fs_at(d)), device_id_type=MESH)

    def spread(g, d):
        return pltpu.make_async_remote_copy(
            src_ref=rbuf.at[g, rep], dst_ref=rbuf.at[g, rep], send_sem=r_ssem.at[g, d - 1],
            recv_sem=r_rsem.at[g, d - 1], device_id=(rep_at(d), fs), device_id_type=MESH)

    for d in range(1, n_fsdp):
        gather(d).start()

    length = len_ref[0]
    lanes = PAIR * HEAD_DIM if rows == HEAD_DIM else PAIR * rows
    lane = lax.broadcasted_iota(jnp.int32, (rows, lanes), 1)
    pos = lax.rem(lane, rows)
    causal = lax.broadcasted_iota(jnp.int32, (rows, lanes), 0) <= pos
    live = lax.rem(lax.broadcasted_iota(jnp.int32, (1, lanes), 1), rows) < length
    low_half = lax.broadcasted_iota(jnp.int32, (lanes, HEAD_DIM), 1) < HEAD_DIM // 2
    minus = jnp.full((prefix + rows, HEAD_DIM), -1.0, BF16)

    for d in range(1, n_fsdp):
        own = kvp.at[fs_at(n_fsdp - d)]
        pltpu.make_async_copy(own, own, ag_recv.at[d - 1]).wait()

    def reduce_rows(g):
        for d in range(1, n_fsdp):
            slot = zrecv.at[g, fs_at(n_fsdp - d)]
            pltpu.make_async_copy(slot, slot, z_rsem.at[g, d - 1]).wait()
        zrecv[g, fs] = zsend[g, fs]
        total = zrecv[g, 0]
        for i in range(1, n_fsdp):
            total = total + zrecv[g, i]
        rbuf[g, rep] = total
        for d in range(1, n_rep):
            spread(g, d).start()

    def group(g, carry):
        for i, (_, dst, _) in enumerate(loads):
            pltpu.make_async_copy(dst.at[g], dst.at[g], in_sem.at[g, i]).wait()
        keys = jnp.concatenate([kvp[:, g, 0].reshape(prefix, HEAD_DIM), kb[g]], axis=0)
        values = jnp.concatenate([kvp[:, g, 1].reshape(prefix, HEAD_DIM), vb[g]], axis=0)
        values_ext = jnp.concatenate([values, minus], axis=1)

        def heads(ref, first, count):
            return jnp.concatenate(
                [ref[g, :, h * HEAD_DIM:(h + 1) * HEAD_DIM] for h in range(first, first + count)],
                axis=0)

        for c in range(GROUP // PAIR):
            q = heads(qb, c * PAIR, PAIR)
            do = heads(db, c * PAIR, PAIR)
            o = heads(ob, c * PAIR, PAIR)
            prod = do.astype(F32) * o.astype(F32)
            both = prod + pltpu.roll(prod, HEAD_DIM // 2, 1)
            rest = both - both.astype(BF16).astype(F32)
            delta = jnp.where(low_half, both, rest).astype(BF16)
            s = dot(keys, q, ((1,), (1,)))
            dp = dot(values_ext, jnp.concatenate([do, delta], axis=1), ((1,), (1,)))
            s = jnp.concatenate(
                [s[:prefix], jnp.where(causal, s[prefix:], MASKED)], axis=0)
            top = jnp.max(s, axis=0, keepdims=True)
            e = jnp.exp((s - top) * SCALE)
            inv = jnp.where(live, 1.0 / jnp.sum(e, axis=0, keepdims=True), 0.0)
            p = e * inv
            prob[:, c * lanes:(c + 1) * lanes] = p.astype(BF16)
            ds = (p * dp).astype(BF16)
            score[:, c * lanes:(c + 1) * lanes] = ds
            dq = (dot(ds, keys, ((0,), (0,))) * SCALE).astype(BF16)
            for j in range(PAIR):
                at = pl.multiple_of(g * WIDTH + (c * PAIR + j) * HEAD_DIM, HEAD_DIM)
                qg_out[:, pl.ds(at, HEAD_DIM)] = dq[j * rows:(j + 1) * rows]
        dv = dot(prob[...], heads(db, 0, GROUP), ((1,), (0,)))
        dk = dot(score[...], heads(qb, 0, GROUP), ((1,), (0,))) * SCALE
        zsend[g, :, 0] = dk[:prefix].reshape(n_fsdp, pre_rows, HEAD_DIM)
        zsend[g, :, 1] = dv[:prefix].reshape(n_fsdp, pre_rows, HEAD_DIM)
        for d in range(1, n_fsdp):
            scatter(g, d).start()
        at = pl.multiple_of(g * HEAD_DIM, HEAD_DIM)
        kg_out[:, pl.ds(at, HEAD_DIM)] = dk[prefix:].astype(BF16)
        vg_out[:, pl.ds(at, HEAD_DIM)] = dv[prefix:].astype(BF16)

        @pl.when(g >= LAG)
        def _():
            reduce_rows(g - LAG)

        return carry

    lax.fori_loop(0, KV_HEADS, group, 0)
    for g in range(KV_HEADS - LAG, KV_HEADS):
        reduce_rows(g)
    for g in range(KV_HEADS):
        for d in range(1, n_rep):
            slot = rbuf.at[g, rep_at(n_rep - d)]
            pltpu.make_async_copy(slot, slot, r_rsem.at[g, d - 1]).wait()
        total = rbuf[g, 0]
        for i in range(1, n_rep):
            total = total + rbuf[g, i]
        pk_out[:, g * HEAD_DIM:(g + 1) * HEAD_DIM] = total[0]
        pv_out[:, g * HEAD_DIM:(g + 1) * HEAD_DIM] = total[1]
    for d in range(1, n_fsdp):
        gather(d).wait_send()
    for g in range(KV_HEADS):
        for d in range(1, n_fsdp):
            scatter(g, d).wait_send()
        for d in range(1, n_rep):
            spread(g, d).wait_send()


def write_out(*refs):
    sems = refs[-1]
    copies = [pltpu.make_async_copy(refs[i], refs[5 + i], sems.at[i]) for i in range(5)]
    for copy in copies:
        copy.start()
    for copy in copies:
        copy.wait()


def on_device(n_rep, n_fsdp, q, k, v, o, do, lengths, pk, pv):
    rows = q.shape[0]
    pre_rows = pk.shape[0]
    keys = n_fsdp * pre_rows + rows
    any_ = pl.BlockSpec(memory_space=pl.ANY)
    vmem = pl.BlockSpec(memory_space=pltpu.VMEM)
    dma = pltpu.SemaphoreType.DMA
    piece = (2, pre_rows, HEAD_DIM)
    held = pl.pallas_call(
        functools.partial(kernel, n_rep, n_fsdp),
        out_shape=(
            pltpu.VMEM(q.shape, BF16),
            pltpu.VMEM(k.shape, BF16),
            pltpu.VMEM(v.shape, BF16),
            pltpu.VMEM(pk.shape, F32),
            pltpu.VMEM(pv.shape, F32),
        ),
        in_specs=[any_] * 5 + [pl.BlockSpec(memory_space=pltpu.SMEM)] + [any_] * 2,
        out_specs=(vmem,) * 5,
        scratch_shapes=[
            pltpu.VMEM((KV_HEADS, rows, WIDTH), BF16),
            pltpu.VMEM((KV_HEADS, rows, WIDTH), BF16),
            pltpu.VMEM((KV_HEADS, rows, WIDTH), BF16),
            pltpu.VMEM((KV_HEADS, rows, HEAD_DIM), BF16),
            pltpu.VMEM((KV_HEADS, rows, HEAD_DIM), BF16),
            pltpu.VMEM((n_fsdp, KV_HEADS) + piece, BF16),
            pltpu.VMEM((keys, GROUP * rows), BF16),
            pltpu.VMEM((keys, GROUP * rows), BF16),
            pltpu.VMEM((KV_HEADS, n_fsdp) + piece, F32),
            pltpu.VMEM((KV_HEADS, n_fsdp) + piece, F32),
            pltpu.VMEM((KV_HEADS, n_rep) + piece, F32),
            dma((KV_HEADS, 5)),
            dma((2, KV_HEADS)),
            dma((n_fsdp - 1,)),
            dma((n_fsdp - 1,)),
            dma((KV_HEADS, n_fsdp - 1)),
            dma((KV_HEADS, n_fsdp - 1)),
            dma((KV_HEADS, n_rep - 1)),
            dma((KV_HEADS, n_rep - 1)),
        ],
        compiler_params=pltpu.CompilerParams(collective_id=0, has_side_effects=True),
    )(q, k, v, o, do, lengths, pk, pv)
    return pl.pallas_call(
        write_out,
        out_shape=tuple(jax.ShapeDtypeStruct(x.shape, x.dtype) for x in held),
        in_specs=[vmem] * 5,
        out_specs=(any_,) * 5,
        scratch_shapes=[dma((5,))],
    )(*[pltpu.with_memory_space_constraint(x, pltpu.VMEM) for x in held])


def solution(mesh):
    wide = P(("rep", "fsdp"), None)
    return jax.shard_map(
        functools.partial(on_device, mesh.shape["rep"], mesh.shape["fsdp"]),
        mesh=mesh,
        in_specs=(wide,) * 5 + (P(("rep", "fsdp")), P("fsdp", None), P("fsdp", None)),
        out_specs=(wide,) * 3 + (P("fsdp", None), P("fsdp", None)),
        check_vma=False,
    )
```

```python
import functools

import jax
import jax.numpy as jnp
from jax import lax
from jax.experimental import pallas as pl
from jax.experimental.pallas import tpu as pltpu
from jax.sharding import PartitionSpec as P

HEAD_DIM = 128
Q_HEADS = 32
KV_HEADS = 4
GROUP = Q_HEADS // KV_HEADS
WIDTH = GROUP * HEAD_DIM
SCALE = HEAD_DIM ** (-0.5)
MASKED = -1e30
PAIR = 2

MESH = pl.DeviceIdType.MESH
F32 = jnp.float32
BF16 = jnp.bfloat16


def dot(a, b, contract):
    return lax.dot_general(a, b, (contract, ((), ())), preferred_element_type=F32)


def kernel(
    n_rep, n_fsdp,
    q_hbm, k_hbm, v_hbm, o_hbm, do_hbm, len_ref, pk_hbm, pv_hbm,
    qg_out, kg_out, vg_out, pk_out, pv_out,
    qb, ob, db, kb, vb, kvp, own_e, own_dp, delta_b, stats, prob, score,
    part, pairb, zsend, zrecv, rbuf,
    in_sem, pre_sem, ag_send, ag_recv, p_ssem, p_rsem, z_ssem, z_rsem, r_ssem, r_rsem,
):
    rep, fs = lax.axis_index("rep"), lax.axis_index("fsdp")
    rows = qb.shape[1]
    pre_rows = kvp.shape[3]
    prefix = n_fsdp * pre_rows
    kind = lax.rem(rep, 2)

    def rep_at(d):
        return lax.rem(rep + d, n_rep)

    def fs_at(d):
        return lax.rem(fs + d, n_fsdp)

    for i, src in enumerate((pk_hbm, pv_hbm)):
        for g in range(KV_HEADS):
            pltpu.make_async_copy(
                src.at[:, pl.ds(g * HEAD_DIM, HEAD_DIM)], kvp.at[fs, g, i], pre_sem.at[i, g]
            ).start()
    barrier = pltpu.get_barrier_semaphore()
    for d in range(1, n_fsdp):
        pl.semaphore_signal(barrier, inc=1, device_id=(rep, fs_at(d)), device_id_type=MESH)
    for d in range(1, n_rep):
        pl.semaphore_signal(barrier, inc=1, device_id=(rep_at(d), fs), device_id_type=MESH)
    loads = ((q_hbm, qb, WIDTH), (do_hbm, db, WIDTH), (o_hbm, ob, WIDTH),
             (k_hbm, kb, HEAD_DIM), (v_hbm, vb, HEAD_DIM))
    for g in range(KV_HEADS):
        for i, (src, dst, width) in enumerate(loads):
            pltpu.make_async_copy(
                src.at[:, pl.ds(g * width, width)], dst.at[g], in_sem.at[g, i]
            ).start()
    for i in range(2):
        for g in range(KV_HEADS):
            pltpu.make_async_copy(kvp.at[fs, g, i], kvp.at[fs, g, i], pre_sem.at[i, g]).wait()
    pl.semaphore_wait(barrier, n_fsdp + n_rep - 2)

    def gather(d):
        return pltpu.make_async_remote_copy(
            src_ref=kvp.at[fs], dst_ref=kvp.at[fs], send_sem=ag_send.at[d - 1],
            recv_sem=ag_recv.at[d - 1], device_id=(rep, fs_at(d)), device_id_type=MESH)

    def swap(g):
        return pltpu.make_async_remote_copy(
            src_ref=part.at[g, 1 - kind], dst_ref=pairb.at[g], send_sem=p_ssem.at[g],
            recv_sem=p_rsem.at[g], device_id=(rep + 1 - 2 * kind, fs), device_id_type=MESH)

    def scatter(g, d):
        return pltpu.make_async_remote_copy(
            src_ref=zsend.at[g, fs_at(d)], dst_ref=zrecv.at[g, fs], send_sem=z_ssem.at[g, d - 1],
            recv_sem=z_rsem.at[g, d - 1], device_id=(rep, fs_at(d)), device_id_type=MESH)

    def spread(g, d):
        return pltpu.make_async_remote_copy(
            src_ref=rbuf.at[g, rep], dst_ref=rbuf.at[g, rep], send_sem=r_ssem.at[g, d - 1],
            recv_sem=r_rsem.at[g, d - 1], device_id=(rep_at(d), fs), device_id_type=MESH)

    for d in range(1, n_fsdp):
        gather(d).start()

    length = len_ref[0]
    lanes = PAIR * rows
    pos = lax.rem(lax.broadcasted_iota(jnp.int32, (rows, lanes), 1), rows)
    causal = lax.broadcasted_iota(jnp.int32, (rows, lanes), 0) <= pos
    live = lax.rem(lax.broadcasted_iota(jnp.int32, (1, lanes), 1), rows) < length
    low_half = lax.broadcasted_iota(jnp.int32, (lanes, HEAD_DIM), 1) < HEAD_DIM // 2

    def heads(ref, g, first, count):
        return jnp.concatenate(
            [ref[g, :, h * HEAD_DIM:(h + 1) * HEAD_DIM] for h in range(first, first + count)],
            axis=0)

    def own_keys(g, carry):
        for i, (_, dst, _) in enumerate(loads):
            pltpu.make_async_copy(dst.at[g], dst.at[g], in_sem.at[g, i]).wait()
        keys = kb[g]
        values = jnp.concatenate([vb[g], jnp.full((rows, HEAD_DIM), -1.0, BF16)], axis=1)
        for c in range(GROUP // PAIR):
            at = slice(c * lanes, (c + 1) * lanes)
            q = heads(qb, g, c * PAIR, PAIR)
            do = heads(db, g, c * PAIR, PAIR)
            o = heads(ob, g, c * PAIR, PAIR)
            prod = do.astype(F32) * o.astype(F32)
            both = prod + pltpu.roll(prod, HEAD_DIM // 2, 1)
            rest = both - both.astype(BF16).astype(F32)
            delta = jnp.where(low_half, both, rest).astype(BF16)
            delta_b[g, at] = delta
            s = jnp.where(causal, dot(keys, q, ((1,), (1,))), MASKED)
            top = jnp.max(s, axis=0, keepdims=True)
            e = jnp.exp((s - top) * SCALE)
            own_e[g, :, at] = e
            stats[g, 0:1, at] = top
            stats[g, 1:2, at] = jnp.sum(e, axis=0, keepdims=True)
            own_dp[g, :, at] = dot(
                values, jnp.concatenate([do, delta], axis=1), ((1,), (1,)))
        return carry

    lax.fori_loop(0, KV_HEADS, own_keys, 0)

    for d in range(1, n_fsdp):
        slot = kvp.at[fs_at(n_fsdp - d)]
        pltpu.make_async_copy(slot, slot, ag_recv.at[d - 1]).wait()

    def add_pair(g):
        pltpu.make_async_copy(pairb.at[g], pairb.at[g], p_rsem.at[g]).wait()
        zsend[g] = part[g, kind] + pairb[g]
        for d in range(1, n_fsdp):
            scatter(g, d).start()

    def add_rows(g):
        for d in range(1, n_fsdp):
            slot = zrecv.at[g, fs_at(n_fsdp - d)]
            pltpu.make_async_copy(slot, slot, z_rsem.at[g, d - 1]).wait()
        zrecv[g, fs] = zsend[g, fs]
        total = zrecv[g, 0]
        for i in range(1, n_fsdp):
            total = total + zrecv[g, i]
        rbuf[g, rep] = total
        for d in range(1, n_rep):
            spread(g, d).start()

    def prefix_keys(g, carry):
        keys = kvp[:, g, 0].reshape(prefix, HEAD_DIM)
        values = jnp.concatenate(
            [kvp[:, g, 1].reshape(prefix, HEAD_DIM), jnp.full((prefix, HEAD_DIM), -1.0, BF16)],
            axis=1)
        for c in range(GROUP // PAIR):
            at = slice(c * lanes, (c + 1) * lanes)
            q = heads(qb, g, c * PAIR, PAIR)
            do = heads(db, g, c * PAIR, PAIR)
            s = dot(keys, q, ((1,), (1,)))
            dp = dot(values, jnp.concatenate([do, delta_b[g, at]], axis=1), ((1,), (1,)))
            own_top = stats[g, 0:1, at]
            top = jnp.maximum(jnp.max(s, axis=0, keepdims=True), own_top)
            e = jnp.exp((s - top) * SCALE)
            shrink = jnp.exp((own_top - top) * SCALE)
            total = jnp.sum(e, axis=0, keepdims=True) + stats[g, 1:2, at] * shrink
            inv = jnp.where(live, 1.0 / total, 0.0)
            p = e * inv
            stats[g, 2:3, at] = shrink * inv
            prob[g, :prefix, at] = p.astype(BF16)
            score[g, :prefix, at] = (p * dp).astype(BF16)
        dk = dot(score[g, :prefix], heads(qb, g, 0, GROUP), ((1,), (0,))) * SCALE
        dv = dot(prob[g, :prefix], heads(db, g, 0, GROUP), ((1,), (0,)))
        part[g, 0] = dk.reshape(n_fsdp, pre_rows, HEAD_DIM)
        part[g, 1] = dv.reshape(n_fsdp, pre_rows, HEAD_DIM)
        swap(g).start()

        @pl.when(g >= 1)
        def _():
            add_pair(g - 1)

        return carry

    lax.fori_loop(0, KV_HEADS, prefix_keys, 0)

    def own_grads(g, carry):
        keys = jnp.concatenate([kvp[:, g, 0].reshape(prefix, HEAD_DIM), kb[g]], axis=0)
        for c in range(GROUP // PAIR):
            at = slice(c * lanes, (c + 1) * lanes)
            p = own_e[g, :, at] * stats[g, 2:3, at]
            prob[g, prefix:, at] = p.astype(BF16)
            score[g, prefix:, at] = (p * own_dp[g, :, at]).astype(BF16)
            dq = (dot(score[g, :, at], keys, ((0,), (0,))) * SCALE).astype(BF16)
            for j in range(PAIR):
                to = pl.multiple_of(g * WIDTH + (c * PAIR + j) * HEAD_DIM, HEAD_DIM)
                qg_out[:, pl.ds(to, HEAD_DIM)] = dq[j * rows:(j + 1) * rows]
        dk = dot(score[g, prefix:], heads(qb, g, 0, GROUP), ((1,), (0,))) * SCALE
        dv = dot(prob[g, prefix:], heads(db, g, 0, GROUP), ((1,), (0,)))
        to = pl.multiple_of(g * HEAD_DIM, HEAD_DIM)
        kg_out[:, pl.ds(to, HEAD_DIM)] = dk.astype(BF16)
        vg_out[:, pl.ds(to, HEAD_DIM)] = dv.astype(BF16)

        @pl.when(g == 0)
        def _():
            add_pair(KV_HEADS - 1)

        @pl.when((g >= 1) & (g <= KV_HEADS // 2))
        def _():
            add_rows(2 * g - 2)
            add_rows(2 * g - 1)

        return carry

    lax.fori_loop(0, KV_HEADS, own_grads, 0)

    for g in range(KV_HEADS):
        for d in range(1, n_rep):
            slot = rbuf.at[g, rep_at(n_rep - d)]
            pltpu.make_async_copy(slot, slot, r_rsem.at[g, d - 1]).wait()
        for first, out in ((0, pk_out), (1, pv_out)):
            total = rbuf[g, first]
            for i in range(first + 2, n_rep, 2):
                total = total + rbuf[g, i]
            out[:, g * HEAD_DIM:(g + 1) * HEAD_DIM] = total
    for d in range(1, n_fsdp):
        gather(d).wait_send()
    for g in range(KV_HEADS):
        swap(g).wait_send()
        for d in range(1, n_fsdp):
            scatter(g, d).wait_send()
        for d in range(1, n_rep):
            spread(g, d).wait_send()


def write_out(*refs):
    sems = refs[-1]
    copies = [pltpu.make_async_copy(refs[i], refs[5 + i], sems.at[i]) for i in range(5)]
    for copy in copies:
        copy.start()
    for copy in copies:
        copy.wait()


def on_device(n_rep, n_fsdp, q, k, v, o, do, lengths, pk, pv):
    rows = q.shape[0]
    pre_rows = pk.shape[0]
    keys = n_fsdp * pre_rows + rows
    any_ = pl.BlockSpec(memory_space=pl.ANY)
    vmem = pl.BlockSpec(memory_space=pltpu.VMEM)
    dma = pltpu.SemaphoreType.DMA
    piece = (pre_rows, HEAD_DIM)
    held = pl.pallas_call(
        functools.partial(kernel, n_rep, n_fsdp),
        out_shape=(
            pltpu.VMEM(q.shape, BF16),
            pltpu.VMEM(k.shape, BF16),
            pltpu.VMEM(v.shape, BF16),
            pltpu.VMEM(pk.shape, F32),
            pltpu.VMEM(pv.shape, F32),
        ),
        in_specs=[any_] * 5 + [pl.BlockSpec(memory_space=pltpu.SMEM)] + [any_] * 2,
        out_specs=(vmem,) * 5,
        scratch_shapes=[
            pltpu.VMEM((KV_HEADS, rows, WIDTH), BF16),
            pltpu.VMEM((KV_HEADS, rows, WIDTH), BF16),
            pltpu.VMEM((KV_HEADS, rows, WIDTH), BF16),
            pltpu.VMEM((KV_HEADS, rows, HEAD_DIM), BF16),
            pltpu.VMEM((KV_HEADS, rows, HEAD_DIM), BF16),
            pltpu.VMEM((n_fsdp, KV_HEADS, 2) + piece, BF16),
            pltpu.VMEM((KV_HEADS, rows, GROUP * rows), F32),
            pltpu.VMEM((KV_HEADS, rows, GROUP * rows), F32),
            pltpu.VMEM((KV_HEADS, GROUP * rows, HEAD_DIM), BF16),
            pltpu.VMEM((KV_HEADS, 8, GROUP * rows), F32),
            pltpu.VMEM((KV_HEADS, keys, GROUP * rows), BF16),
            pltpu.VMEM((KV_HEADS, keys, GROUP * rows), BF16),
            pltpu.VMEM((KV_HEADS, 2, n_fsdp) + piece, F32),
            pltpu.VMEM((KV_HEADS, n_fsdp) + piece, F32),
            pltpu.VMEM((KV_HEADS, n_fsdp) + piece, F32),
            pltpu.VMEM((KV_HEADS, n_fsdp) + piece, F32),
            pltpu.VMEM((KV_HEADS, n_rep) + piece, F32),
            dma((KV_HEADS, 5)),
            dma((2, KV_HEADS)),
            dma((n_fsdp - 1,)),
            dma((n_fsdp - 1,)),
            dma((KV_HEADS,)),
            dma((KV_HEADS,)),
            dma((KV_HEADS, n_fsdp - 1)),
            dma((KV_HEADS, n_fsdp - 1)),
            dma((KV_HEADS, n_rep - 1)),
            dma((KV_HEADS, n_rep - 1)),
        ],
        compiler_params=pltpu.CompilerParams(collective_id=0, has_side_effects=True),
    )(q, k, v, o, do, lengths, pk, pv)
    return pl.pallas_call(
        write_out,
        out_shape=tuple(jax.ShapeDtypeStruct(x.shape, x.dtype) for x in held),
        in_specs=[vmem] * 5,
        out_specs=(any_,) * 5,
        scratch_shapes=[dma((5,))],
    )(*[pltpu.with_memory_space_constraint(x, pltpu.VMEM) for x in held])


def solution(mesh):
    wide = P(("rep", "fsdp"), None)
    return jax.shard_map(
        functools.partial(on_device, mesh.shape["rep"], mesh.shape["fsdp"]),
        mesh=mesh,
        in_specs=(wide,) * 5 + (P(("rep", "fsdp")), P("fsdp", None), P("fsdp", None)),
        out_specs=(wide,) * 3 + (P("fsdp", None), P("fsdp", None)),
        check_vma=False,
    )
```
